32 devices in a mesh: cp: 16 (over z, x, core), tp: 2 (over y).
Axes of the slice: x: 2, y: 2, z: 4, core: 2. Of those that a mesh axis runs over, the one named last changes fastest.
Arguments:
- hidden: bfloat16 [8192, 4096], P('cp', 'tp'), may hold values from -6 to 6
- norm_gain: float32 [4096], replicated, may hold values from 0.5 to 1.5
- w_query: bfloat16 [4096, 4096], P(None, 'tp'), may hold values from -0.140625 to 0.140625
- w_key: bfloat16 [4096, 1024], P(None, 'tp'), may hold values from -4 to 4
- w_value: bfloat16 [4096, 1024], P(None, 'tp'), may hold values from -0.09375 to 0.09375
- w_out: bfloat16 [4096, 4096], P('tp'), may hold values from -0.5 to 0.5
- doc_ids: int32 [8192], P('cp'), may hold values from 0 to 5, never falling along the last dimension, each value on 1 to 6144 neighbouring positions
Outputs:
- updated: bfloat16 [8192, 4096], P('cp', 'tp')
The draws below stay inside these ranges and needn't reach their ends.
Inputs may be any that keep to these rules, and one draw needn't show every extreme that they name: `doc_ids`: document numbers never fall along the sequence; every document has 1 to 6144 tokens.
All inputs are finite; a program needn't handle non-finite values.
Results may differ from the reference program's by a relative error of at most 0.017.
The reference program's roundings to bfloat16 on the way count: a program that leaves them out, or rounds other values in their place, can miss the bound.
Values may be sent and summed in bfloat16 or wider, within the bound.
A program may use at most 128 MiB of HBM per device.

```python
import math
import jax
import jax.numpy as jnp
import numpy as np
from jax import lax

D = 4096
HEADS = 32
KV_HEADS = 8
HEAD_SIZE = 128
TOK_DEV = 512
DOCS = 6
SEQ = 8192
LONGEST = 6144
N_TP = 2


def query_key_pair(key):
    spread = 1.5 / math.sqrt(D)
    limit = 9.0 / math.sqrt(D)
    base = jax.random.normal(jax.random.fold_in(key, 101), (D, HEADS * HEAD_SIZE), jnp.float32) * spread
    base = jnp.clip(base, -limit, limit)
    other = jax.random.normal(jax.random.fold_in(key, 202), (D, KV_HEADS * HEAD_SIZE), jnp.float32) * spread
    other = jnp.clip(other, -limit, limit)
    return (base, other)


def draw_w_query(key, part):
    base, other = query_key_pair(key)
    return base.astype(jnp.bfloat16)


def draw_w_key(key, part):
    base, other = query_key_pair(key)
    result = other
    return result.astype(jnp.bfloat16)


def block_levels(rng, dims, cuts, low, top_value):
    loudness = 1.0
    for axis_at, shards_of in cuts:
        draws = jax.random.uniform(jax.random.fold_in(jax.random.fold_in(rng, 6), axis_at), (shards_of,), jnp.float32, low / len(cuts), top_value / len(cuts))
        loudness = loudness * jnp.repeat(jnp.exp(draws), dims[axis_at] // shards_of).reshape((-1,) + (1,) * (len(dims) - 1 - axis_at))
    return loudness


def length_profile(amount, total, reach, slope):
    loads = [(1 << 20) // math.isqrt(standing ** slope) + 1 for standing in range(2, amount + 1)]
    rest, given = total - reach - (amount - 1), [1] * (amount - 1)
    while rest > 0:
        free = [i for i in range(amount - 1) if given[i] < reach]
        whole, remaining = sum([loads[i] for i in free]), rest
        for i in free:
            addition = min(reach - given[i], max(1, remaining * loads[i] // whole), rest)
            given[i] = given[i] + addition
            rest = rest - addition
    return np.array([reach] + given)


def uneven(own_key, number_of, total, reach, skew):
    if number_of == 2:
        one = jax.random.randint(own_key, (), max(1, total - reach), min(reach, total - 1) + 1)
        return jnp.stack([one, total - one])
    sizes = jnp.asarray(length_profile(number_of, total, reach, skew), jnp.int32)
    twos = (number_of - 1) // 2
    donor, sink = sizes[1:1 + 2 * twos:2], sizes[2:2 + 2 * twos:2]
    slack = jnp.minimum(donor - 1, reach - sink)
    passed = jax.random.randint(jax.random.fold_in(own_key, 1), (twos,), 0, 1 << 20) % (slack + 1)
    sizes = sizes.at[1:1 + 2 * twos:2].set(donor - passed).at[2:2 + 2 * twos:2].set(sink + passed)
    return sizes[jax.random.permutation(jax.random.fold_in(own_key, 2), number_of)]


def centred(own_key, dims, scale, most, shards=(), held_as=jnp.bfloat16):
    values = scale * jax.random.normal(own_key, dims, jnp.float32)
    if shards:
        values = values * block_levels(own_key, dims, shards, -0.22, 0.18)
    return jnp.clip(values, -most, most).astype(held_as)


def setup_inputs(seed: int = 0) -> dict:
    seeds = jax.random.split(jax.random.key(seed), 8)
    return {
        "hidden": centred(seeds[0], (SEQ, D), 1.0, 6.0, ((0, 16), (1, 2))),
        "norm_gain": jnp.clip(1.0 + 0.1 * jax.random.normal(seeds[1], (D,), jnp.float32), 0.5, 1.5),
        "w_query": draw_w_query(jax.random.fold_in(seeds[7], 71), 0),
        "w_key": draw_w_key(jax.random.fold_in(seeds[7], 71), 0),
        "w_value": centred(seeds[4], (D, KV_HEADS * HEAD_SIZE), D ** -0.5, 0.09375, ((1, 2),)),
        "w_out": centred(seeds[5], (HEADS * HEAD_SIZE, D), (HEADS * HEAD_SIZE // 32) ** -0.5, 0.5, ((0, 2),)),
        "doc_ids": jnp.searchsorted(jnp.cumsum(uneven(seeds[6], DOCS, SEQ, LONGEST, 2)), jnp.arange(SEQ), side="right").astype(jnp.int32),
    }


epsilon = 1e-05
rope_base = 500000.0

def rotate(vectors, positions):
    half = HEAD_SIZE // 2
    freqs = rope_base ** (-jnp.arange(half, dtype=jnp.float32) * 2.0 / HEAD_SIZE)
    angles = positions.astype(jnp.float32)[:, None] * freqs[None, :]
    cosine = jnp.cos(angles)[:, None, :]
    sine = jnp.sin(angles)[:, None, :]
    first = vectors[..., :half]
    second = vectors[..., half:]
    return jnp.concatenate([first * cosine - second * sine, second * cosine + first * sine], axis=-1)

def attend_block(loop_state, query_matrix, query_pos, query_doc, key_matrix, value_matrix, key_pos, key_doc):
    best, total, running_output = loop_state
    logit_matrix = jnp.einsum('ucpm,ycm->cpuy', query_matrix.astype(jnp.float32), key_matrix.astype(jnp.float32)) * HEAD_SIZE ** (-0.5)
    allowed = (key_pos[None, :] <= query_pos[:, None]) & (key_doc[None, :] == query_doc[:, None])
    masked = jnp.where(allowed, logit_matrix, jnp.float32(-1e+30))
    new_best = jnp.maximum(best, lax.optimization_barrier(jnp.max(masked, axis=-1)))
    correction_scale = jnp.exp(best - new_best)
    attention_weights = jnp.where(allowed, jnp.exp(logit_matrix - new_best[..., None]), jnp.float32(0.0))
    total = total * correction_scale + lax.optimization_barrier(jnp.sum(attention_weights, axis=-1))
    rounded_weights = attention_weights.astype(jnp.bfloat16).astype(jnp.float32)
    running_output = running_output * correction_scale[..., None] + jnp.einsum('sfec,csh->sfeh', rounded_weights, value_matrix.astype(jnp.float32))
    return (new_best, total, running_output)

def reference(hidden, norm_gain, w_query, w_key, w_value, w_out, doc_ids):
    seq_len = hidden.shape[0]
    group = HEADS // KV_HEADS
    wide = hidden.astype(jnp.float32)
    inverse_rms = lax.rsqrt(lax.optimization_barrier(jnp.mean(wide * wide, axis=1, keepdims=True)) + epsilon)
    normed = (wide * inverse_rms * norm_gain.astype(jnp.float32)[None, :]).astype(jnp.bfloat16)
    positions = jnp.arange(seq_len, dtype=jnp.int32)
    query_raw = jnp.dot(normed, w_query, preferred_element_type=jnp.float32).reshape(seq_len, HEADS, HEAD_SIZE)
    key_raw = jnp.dot(normed, w_key, preferred_element_type=jnp.float32).reshape(seq_len, KV_HEADS, HEAD_SIZE)
    query_matrix = rotate(query_raw, positions).astype(jnp.bfloat16).reshape(seq_len, KV_HEADS, group, HEAD_SIZE)
    key_matrix = rotate(key_raw, positions).astype(jnp.bfloat16)
    value_matrix = jnp.dot(normed, w_value, preferred_element_type=jnp.float32).astype(jnp.bfloat16).reshape(seq_len, KV_HEADS, HEAD_SIZE)
    block_index = TOK_DEV if TOK_DEV <= 512 else 512
    blocks = seq_len // block_index

    def one_query_block(index):
        start = (index * block_index).astype(jnp.int32)
        query_blk = lax.dynamic_slice_in_dim(query_matrix, start, block_index, 0)
        query_pos = start + jnp.arange(block_index, dtype=jnp.int32)
        query_doc = lax.dynamic_slice_in_dim(doc_ids, start, block_index, 0)

        def loop_body(loop_state, key_block_index):
            key_offset = (key_block_index * block_index).astype(jnp.int32)

            def work(state):
                key_blk = lax.dynamic_slice_in_dim(key_matrix, key_offset, block_index, 0)
                value_blk = lax.dynamic_slice_in_dim(value_matrix, key_offset, block_index, 0)
                key_pos = key_offset + jnp.arange(block_index, dtype=jnp.int32)
                key_doc = lax.dynamic_slice_in_dim(doc_ids, key_offset, block_index, 0)
                return attend_block(state, query_blk, query_pos, query_doc, key_blk, value_blk, key_pos, key_doc)
            return (lax.cond(key_offset <= start + block_index - 1, work, lambda state: state, loop_state), None)
        init = (jnp.full((KV_HEADS, group, block_index), -1e+30, jnp.float32), jnp.zeros((KV_HEADS, group, block_index), jnp.float32), jnp.zeros((KV_HEADS, group, block_index, HEAD_SIZE), jnp.float32))
        final, _ = lax.scan(loop_body, init, jnp.arange(blocks, dtype=jnp.int32))
        result = final[2] / final[1][..., None]
        return jnp.transpose(result, (2, 0, 1, 3)).reshape(block_index, HEADS * HEAD_SIZE).astype(jnp.bfloat16)
    attended = lax.map(one_query_block, jnp.arange(blocks, dtype=jnp.int32)).reshape(seq_len, HEADS * HEAD_SIZE)
    width_cols = HEADS * HEAD_SIZE // N_TP
    mixed = jnp.zeros((seq_len, hidden.shape[1]), jnp.float32)
    for group_index in range(N_TP):
        lower = group_index * width_cols
        partial_sum = jnp.dot(attended[:, lower:lower + width_cols], w_out[lower:lower + width_cols], preferred_element_type=jnp.float32).astype(jnp.bfloat16)
        partial_sum = lax.optimization_barrier(partial_sum)
        mixed = mixed + partial_sum.astype(jnp.float32)
    return mixed.astype(jnp.bfloat16)
```

```python
import functools

import jax
import jax.numpy as jnp
from jax import lax
from jax.experimental import pallas as pl
from jax.experimental.pallas import tpu as pltpu
from jax.sharding import PartitionSpec as P

HEADS = 32
KV_HEADS = 8
HEAD_SIZE = 128
GROUP = HEADS // KV_HEADS

epsilon = 1e-05
rope_base = 500000.0
LOG2E = 1.4426950408889634
SCALE = HEAD_SIZE ** (-0.5) * LOG2E
FLOOR = -1e29
MASKED = -1e30
CHUNK = 128
QTILE = 128
NEAR = 8
LANES = 128
MESH = pl.DeviceIdType.MESH


def tables(positions):
    half = HEAD_SIZE // 2
    freqs = rope_base ** (-jnp.arange(half, dtype=jnp.float32) * 2.0 / HEAD_SIZE)
    angles = positions.astype(jnp.float32)[:, None] * freqs[None, :]
    cosine = jnp.cos(angles)
    sine = jnp.sin(angles)
    return (
        jnp.concatenate([cosine, cosine], axis=1),
        jnp.concatenate([-sine, sine], axis=1),
    )


def columns_of(n_cp):
    chips = n_cp // 2
    cols = 1
    while cols * cols * 4 <= chips:
        cols *= 2
    return cols


def layer_kernel(
    hid_hbm, gain_ref, wq_hbm, wk_hbm, wv_hbm, wo_hbm, cos_ref, sin_ref, docs_ref, qdoc_ref,
    out_hbm,
    hid, wq, wkv, kv, q, normed, acc, ml, docs, recv, stage,
    hid_send, hid_recv, own_sem, w_sem, doc_send, doc_recv, kv_send, kv_recv,
    part_send, part_recv, out_sem,
    *, n_cp, n_tp, longest,
):
    tok, feat = hid_hbm.shape
    width = gain_ref.shape[1]
    q_cols = wq.shape[1]
    kv_cols = wkv.shape[1]
    n_kv = kv_cols // (2 * HEAD_SIZE)
    chunks = tok // CHUNK
    n_tiles = tok // QTILE
    cols = columns_of(n_cp)
    rows_z = n_cp // (2 * cols)
    window = min((longest + tok - 2) // tok, n_cp - 1)
    chip_window = (window + 1) // 2
    near = min(NEAR, window + 1)

    me = lax.axis_index("cp")
    rank = lax.axis_index("tp")
    core = lax.rem(me, 2)
    my_x = lax.rem(me // 2, cols)
    my_z = me // (2 * cols)

    def peer_of(by):
        return lax.rem(rank + by, n_tp)

    barrier = pltpu.get_barrier_semaphore()
    for by in range(1, n_tp):
        pl.semaphore_signal(barrier, inc=1, device_id={"tp": peer_of(by)}, device_id_type=MESH)

    def greet(by, carry):
        pl.semaphore_signal(
            barrier, inc=1, device_id={"cp": lax.rem(me + by, n_cp)}, device_id_type=MESH
        )
        return carry

    lax.fori_loop(1, n_cp, greet, 0)

    wk_copy = pltpu.make_async_copy(wk_hbm, wkv.at[:, pl.ds(0, kv_cols // 2)], w_sem.at[0])
    wv_copy = pltpu.make_async_copy(
        wv_hbm, wkv.at[:, pl.ds(kv_cols // 2, kv_cols // 2)], w_sem.at[1]
    )
    wq_copy = pltpu.make_async_copy(wq_hbm, wq, w_sem.at[2])
    own_copy = pltpu.make_async_copy(hid_hbm, hid.at[rank], own_sem)
    own_copy.start()
    wk_copy.start()
    wv_copy.start()
    wq_copy.start()
    docs[me] = docs_ref[...]
    pl.semaphore_wait(barrier, n_cp - 1 + n_tp - 1)

    def hid_copy(by, t):
        rows = pl.ds(t * CHUNK, CHUNK)
        return pltpu.make_async_remote_copy(
            src_ref=hid_hbm.at[rows],
            dst_ref=hid.at[rank, rows],
            send_sem=hid_send.at[by - 1, t],
            recv_sem=hid_recv.at[n_tp - 1 - by, t],
            device_id={"tp": peer_of(by)},
            device_id_type=MESH,
        )

    for t in range(chunks):
        for by in range(1, n_tp):
            hid_copy(by, t).start()

    def doc_copy(source, target):
        return pltpu.make_async_remote_copy(
            src_ref=docs_ref,
            dst_ref=docs.at[source],
            send_sem=doc_send.at[target],
            recv_sem=doc_recv.at[source],
            device_id={"cp": target},
            device_id_type=MESH,
        )

    last_target = jnp.minimum(me + window, n_cp - 1)

    def doc_start(target, carry):
        doc_copy(me, target).start()
        return carry

    lax.fori_loop(me + 1, last_target + 1, doc_start, 0)

    def takes(z, x, zs, xs):
        reach = z * cols - (zs * cols + xs) <= chip_window
        by_z = (xs == x) & (zs < z) & reach
        from_left = (xs < x) & (zs <= z) & (z * cols + x - (zs * cols + xs) <= chip_window)
        from_right = (xs > x) & (zs < z) & reach
        return by_z | from_left | from_right

    def block_copy(direction, zs, xs, ks, t, target):
        chip = zs * cols + xs
        s = chip * 2 + ks
        rows = pl.ds(pl.multiple_of(s * tok + t * CHUNK, CHUNK), CHUNK)
        return pltpu.make_async_remote_copy(
            src_ref=kv.at[rows],
            dst_ref=kv.at[rows],
            send_sem=kv_send.at[direction, chip * chunks + t],
            recv_sem=kv_recv.at[s * chunks + t],
            device_id={"cp": target},
            device_id_type=MESH,
        )

    def hops(zs, xs):
        own_chip = (zs == my_z) & (xs == my_x)
        return (
            ((xs == my_x) & (my_z + 1 < rows_z) & takes(my_z + 1, my_x, zs, xs), me + 2 * cols),
            ((xs <= my_x) & (my_x + 1 < cols) & takes(my_z, my_x + 1, zs, xs), me + 2),
            ((xs >= my_x) & (my_x >= 1) & takes(my_z, my_x - 1, zs, xs), me - 2),
            (jnp.logical_not(own_chip) | (core == 0), me + 1 - 2 * core),
        )

    def forward(zs, xs, t):
        for direction, (wanted, target) in enumerate(hops(zs, xs)):
            @pl.when(wanted)
            def _():
                block_copy(direction, zs, xs, core, t, target).start()

    def arrive(zs, xs, ks, t, relay):
        in_range = (zs >= 0) & (xs >= 0) & (xs < cols) & (t >= 0) & (t < chunks)
        own_chip = (zs == my_z) & (xs == my_x)
        if relay:
            wanted = in_range & takes(my_z, my_x, zs, xs)
        else:
            wanted = in_range & (takes(my_z, my_x, zs, xs) | (own_chip & (core == 1)))

        @pl.when(wanted)
        def _():
            block_copy(0, zs, xs, ks, t, me).wait_recv()
            if relay:
                forward(zs, xs, t)

    def handle_round(r):
        def along_z(dz, carry):
            arrive(my_z - dz, my_x, core, r - dz, True)
            return carry

        lax.fori_loop(1, rows_z, along_z, 0)
        for dx in range(1, cols):
            def along_x(dz, carry):
                arrive(my_z - dz, my_x - dx, core, r - dz, True)
                arrive(my_z - dz, my_x + dx, core, r - dz, True)
                return carry

            lax.fori_loop(0, rows_z, along_x, 0)

        def along_core(i, carry):
            arrive(my_z - i // cols, lax.rem(i, cols), 1 - core, r - i // cols, False)
            return carry

        lax.fori_loop(0, rows_z * cols, along_core, 0)

    own_copy.wait()
    wk_copy.wait()
    wv_copy.wait()
    part_rows = 32

    def rope(raw, cosine, sine):
        turned = raw * cosine + pltpu.roll(raw, HEAD_SIZE // 2, 1) * sine
        return turned.astype(jnp.bfloat16)

    def chunk_step(t, carry):
        base = pl.multiple_of(t * CHUNK, CHUNK)
        for by in range(1, n_tp):
            pltpu.make_async_remote_copy(
                src_ref=hid.at[peer_of(by), pl.ds(base, CHUNK)],
                dst_ref=hid.at[peer_of(by), pl.ds(base, CHUNK)],
                send_sem=hid_send.at[by - 1, t],
                recv_sem=hid_recv.at[by - 1, t],
                device_id={"tp": peer_of(by)},
                device_id_type=MESH,
            ).wait_recv()

        def norm_part(i, carry):
            rows = pl.ds(pl.multiple_of(base + i * part_rows, part_rows), part_rows)
            total = jnp.zeros((part_rows, LANES), jnp.float32)
            for j in range(n_tp):
                wide = hid[j, rows, :].astype(jnp.float32)
                square = wide * wide
                for c in range(feat // LANES):
                    total = total + square[:, c * LANES : (c + 1) * LANES]
            mean = jnp.sum(total, axis=1, keepdims=True) / width
            inverse_rms = lax.rsqrt(mean + epsilon)
            out_rows = pl.ds(pl.multiple_of(i * part_rows, part_rows), part_rows)
            for j in range(n_tp):
                wide = hid[j, rows, :].astype(jnp.float32)
                gain = gain_ref[:, j * feat : (j + 1) * feat]
                normed[out_rows, j * feat : (j + 1) * feat] = (
                    wide * inverse_rms * gain
                ).astype(jnp.bfloat16)
            return carry

        lax.fori_loop(0, CHUNK // part_rows, norm_part, 0)
        rows = pl.ds(base, CHUNK)
        cosine = cos_ref[rows, :]
        sine = sin_ref[rows, :]
        own_rows = pl.ds(pl.multiple_of(me * tok + t * CHUNK, CHUNK), CHUNK)
        for g in range(2 * n_kv):
            lanes = slice(g * HEAD_SIZE, (g + 1) * HEAD_SIZE)
            if g % 2 == 0:
                pair = jnp.dot(
                    normed[...],
                    wkv[:, g * HEAD_SIZE : (g + 2) * HEAD_SIZE],
                    preferred_element_type=jnp.float32,
                )
            raw = pair[:, (g % 2) * HEAD_SIZE : (g % 2 + 1) * HEAD_SIZE]
            kv[own_rows, lanes] = rope(raw, cosine, sine) if g < n_kv else raw.astype(jnp.bfloat16)

        @pl.when(t == 0)
        def _():
            wq_copy.wait()

        def query_group(g, carry):
            cut = pl.multiple_of(g * GROUP * HEAD_SIZE, HEAD_SIZE)
            raw = jnp.dot(
                normed[...],
                wq[:, pl.ds(cut, GROUP * HEAD_SIZE)],
                preferred_element_type=jnp.float32,
            )
            for h in range(GROUP):
                q[g * GROUP + h, rows, :] = rope(
                    raw[:, h * HEAD_SIZE : (h + 1) * HEAD_SIZE], cosine, sine
                )
            return carry

        query_group(0, 0)
        forward(my_z, my_x, t)
        lax.fori_loop(1, n_kv, query_group, 0)
        handle_round(t - 1)
        return carry

    lax.fori_loop(0, chunks, chunk_step, 0)

    wo_copies = [
        pltpu.make_async_copy(
            wo_hbm.at[:, pl.ds(j * feat, feat)], wq.at[pl.ds(j * q_cols, q_cols)], w_sem.at[3 + j]
        )
        for j in range(n_tp)
    ]
    for copy in wo_copies:
        copy.start()

    strips = feat // LANES
    block_lanes = tok // LANES
    lane = lax.broadcasted_iota(jnp.int32, (QTILE, LANES), 1)
    low_half = lane < LANES // 2

    def doc_strip(s):
        return s // strips, pl.ds(pl.multiple_of(lax.rem(s, strips) * LANES, LANES), LANES)

    def key_docs(s):
        row = jnp.broadcast_to(docs[s], (LANES, tok))
        number = lax.broadcasted_iota(jnp.int32, (LANES, tok), 0)
        one_hot = jnp.where(row == number, 1.0, 0.0).astype(jnp.float32)
        j, lanes = doc_strip(s)
        hid[j, :, lanes] = one_hot.T.astype(jnp.bfloat16)

    def attend(g, tile, s, first):
        key_rows = pl.ds(pl.multiple_of(s * tok, tok), tok)
        j, lanes = doc_strip(s)
        key_lanes = pl.ds(pl.multiple_of(g * HEAD_SIZE, HEAD_SIZE), HEAD_SIZE)
        value_lanes = pl.ds(pl.multiple_of((n_kv + g) * HEAD_SIZE, HEAD_SIZE), HEAD_SIZE)
        keys = jnp.concatenate([kv[key_rows, key_lanes], hid[j, :, lanes]], axis=1)
        values = jnp.concatenate(
            [kv[key_rows, value_lanes], jnp.ones((tok, LANES), jnp.bfloat16)], axis=1
        )
        rows = pl.ds(pl.multiple_of(tile * QTILE, QTILE), QTILE)
        if first:
            row = lax.broadcasted_iota(jnp.int32, (QTILE, LANES), 0) + tile * QTILE
        for h in range(GROUP):
            head = g * GROUP + h
            queries = jnp.concatenate([q[head, rows, :], qdoc_ref[rows, :]], axis=1)
            scores = lax.dot_general(
                queries, keys, (((1,), (1,)), ((), ())), preferred_element_type=jnp.float32
            )
            pieces = [
                scores[:, c * LANES : (c + 1) * LANES] * SCALE for c in range(block_lanes)
            ]
            if first:
                pieces = [
                    jnp.where(row >= lane + c * LANES, p, MASKED) for c, p in enumerate(pieces)
                ]
            top = functools.reduce(jnp.maximum, pieces)
            top = jnp.max(top, axis=1, keepdims=True)
            if first:
                new = jnp.broadcast_to(jnp.maximum(top, FLOOR), (QTILE, LANES))
            else:
                packed = ml[head, rows, :]
                turned = pltpu.roll(packed, LANES // 2, 1)
                old = jnp.where(low_half, packed, turned)
                total = jnp.where(low_half, turned, packed)
                new = jnp.maximum(old, top)
                correction = jnp.exp2(old - new)
            weights = jnp.concatenate(
                [jnp.exp2(p - new).astype(jnp.bfloat16) for p in pieces], axis=1
            )
            sums = jnp.dot(weights, values, preferred_element_type=jnp.float32)
            if first:
                acc[head, rows, :] = sums[:, :HEAD_SIZE]
                ml[head, rows, :] = jnp.where(low_half, new, sums[:, HEAD_SIZE:])
            else:
                acc[head, rows, :] = acc[head, rows, :] * correction + sums[:, :HEAD_SIZE]
                ml[head, rows, :] = jnp.where(
                    low_half, new, total * correction + sums[:, HEAD_SIZE:]
                )

    def all_tiles(s, first):
        def one(i, carry):
            attend(i // n_tiles, lax.rem(i, n_tiles), s, first)
            return carry

        lax.fori_loop(0, n_kv * n_tiles, one, 0)

    key_docs(me)
    all_tiles(me, True)

    in_row = lax.rem(me, 2 * cols) + 1
    last_round = chunks - 1 + rows_z - 1

    def rounds_before(o):
        distance = jnp.where(o < in_row, 0, (o - in_row) // (2 * cols) + 1)
        return jnp.clip(
            jnp.maximum(chunks - 1 + o // 2, chunks - 1 + distance), chunks - 1, last_round
        )

    def take_rounds(begin, end):
        def one(r, carry):
            handle_round(r)
            return carry

        lax.fori_loop(begin, end, one, 0)

    def docs_for(s):
        doc_copy(s, me).wait_recv()
        key_docs(s)

    def near_step(o, carry):
        take_rounds(jnp.where(o == 1, chunks - 1, rounds_before(o - 1) + 1), rounds_before(o) + 1)
        s = me - o

        @pl.when(s >= 0)
        def _():
            docs_for(s)
            all_tiles(s, False)

        return carry

    lax.fori_loop(1, near, near_step, 0)
    take_rounds(rounds_before(near - 1) + 1, last_round + 1)

    def far_docs(o, carry):
        @pl.when(me - o >= 0)
        def _():
            docs_for(me - o)

        return carry

    lax.fori_loop(near, window + 1, far_docs, 0)
    for copy in wo_copies:
        copy.wait()

    far_end = jnp.minimum(window, me) + 1
    col_step = min(512, feat)

    def part_copy(by, tile):
        rows = pl.ds(pl.multiple_of(tile * QTILE, QTILE), QTILE)
        return pltpu.make_async_remote_copy(
            src_ref=stage.at[by - 1, rows],
            dst_ref=recv.at[n_tp - 1 - by, rows],
            send_sem=part_send.at[by - 1, tile],
            recv_sem=part_recv.at[n_tp - 1 - by, tile],
            device_id={"tp": peer_of(by)},
            device_id_type=MESH,
        )

    def tile_step(tile, carry):
        rows = pl.ds(pl.multiple_of(tile * QTILE, QTILE), QTILE)

        def far_step(i, carry):
            attend(lax.rem(i, n_kv), tile, me - near - i // n_kv, False)
            return carry

        lax.fori_loop(0, jnp.maximum(far_end - near, 0) * n_kv, far_step, 0)

        def finish(head, carry):
            packed = ml[head, rows, :]
            total = jnp.where(low_half, pltpu.roll(packed, LANES // 2, 1), packed)
            lanes = pl.ds(pl.multiple_of(head * HEAD_SIZE, HEAD_SIZE), HEAD_SIZE)
            normed[:, lanes] = (acc[head, rows, :] / total).astype(jnp.bfloat16)
            return carry

        lax.fori_loop(0, n_kv * GROUP, finish, 0)
        attended = normed[:, :q_cols]
        for by in list(range(1, n_tp)) + [0]:
            piece = pl.ds(pl.multiple_of(peer_of(by) * q_cols, q_cols), q_cols)
            for c in range(feat // col_step):
                part = jnp.dot(
                    attended,
                    wq[piece, c * col_step : (c + 1) * col_step],
                    preferred_element_type=jnp.float32,
                ).astype(jnp.bfloat16)
                if by:
                    stage[by - 1, rows, c * col_step : (c + 1) * col_step] = part
                else:
                    for h in range(col_step // LANES):
                        q[c * (col_step // LANES) + h, rows, :] = part[
                            :, h * LANES : (h + 1) * LANES
                        ]
        for by in range(1, n_tp):
            part_copy(by, tile).start()
        return carry

    lax.fori_loop(0, n_tiles, tile_step, 0)

    def out_copy(tile):
        rows = pl.ds(pl.multiple_of(tile * QTILE, QTILE), QTILE)
        return pltpu.make_async_copy(recv.at[0, rows], out_hbm.at[rows], out_sem.at[tile])

    def sum_step(tile, carry):
        rows = pl.ds(pl.multiple_of(tile * QTILE, QTILE), QTILE)
        for by in range(1, n_tp):
            part_copy(by, tile).wait_recv()
        for c in range(feat // LANES):
            lanes = slice(c * LANES, (c + 1) * LANES)
            total = q[c, rows, :].astype(jnp.float32)
            for by in range(1, n_tp):
                total = total + recv[by - 1, rows, lanes].astype(jnp.float32)
            recv[0, rows, lanes] = total.astype(jnp.bfloat16)
        out_copy(tile).start()
        return carry

    lax.fori_loop(0, n_tiles, sum_step, 0)

    def sent_step(i, carry):
        t = lax.rem(i, chunks)
        chip = i // chunks
        zs, xs = chip // cols, lax.rem(chip, cols)
        own_chip = (zs == my_z) & (xs == my_x)
        held = own_chip | ((zs <= my_z) & takes(my_z, my_x, zs, xs))
        for direction, (wanted, target) in enumerate(hops(zs, xs)):
            @pl.when(held & wanted)
            def _():
                block_copy(direction, zs, xs, core, t, target).wait_send()

        return carry

    lax.fori_loop(0, n_cp // 2 * chunks, sent_step, 0)

    def doc_sent(target, carry):
        doc_copy(me, target).wait_send()
        return carry

    lax.fori_loop(me + 1, last_target + 1, doc_sent, 0)
    for t in range(chunks):
        for by in range(1, n_tp):
            hid_copy(by, t).wait_send()

    def end_step(tile, carry):
        for by in range(1, n_tp):
            part_copy(by, tile).wait_send()
        out_copy(tile).wait()
        return carry

    lax.fori_loop(0, n_tiles, end_step, 0)


def shards(hidden, norm_gain, w_query, w_key, w_value, w_out, doc_ids, *, n_cp, n_tp):
    tok, feat = hidden.shape
    width = norm_gain.shape[0]
    q_cols = w_query.shape[1]
    kv_cols = 2 * w_key.shape[1]
    seq = tok * n_cp
    longest = seq * 3 // 4
    chunks = tok // CHUNK
    n_tiles = tok // QTILE
    cp_rank = lax.axis_index("cp")
    positions = cp_rank * tok + jnp.arange(tok, dtype=jnp.int32)
    cosine, sine = tables(positions)
    number = jnp.arange(LANES, dtype=jnp.int32)
    other_docs = jnp.where(doc_ids[:, None] == number[None, :], 0.0, MASKED).astype(jnp.bfloat16)
    vmem = pl.BlockSpec(memory_space=pltpu.VMEM)
    hbm = pl.BlockSpec(memory_space=pl.ANY)
    bf16, f32 = jnp.bfloat16, jnp.float32
    dma = pltpu.SemaphoreType.DMA
    heads = q_cols // HEAD_SIZE
    return pl.pallas_call(
        functools.partial(layer_kernel, n_cp=n_cp, n_tp=n_tp, longest=longest),
        out_shape=jax.ShapeDtypeStruct((tok, feat), bf16),
        in_specs=[hbm, vmem, hbm, hbm, hbm, hbm, vmem, vmem, vmem, vmem],
        out_specs=hbm,
        scratch_shapes=[
            pltpu.VMEM((n_tp, tok, feat), bf16),
            pltpu.VMEM((width, q_cols), bf16),
            pltpu.VMEM((width, kv_cols), bf16),
            pltpu.VMEM((seq, kv_cols), bf16),
            pltpu.VMEM((heads, tok, HEAD_SIZE), bf16),
            pltpu.VMEM((CHUNK, width), bf16),
            pltpu.VMEM((heads, tok, HEAD_SIZE), f32),
            pltpu.VMEM((heads, tok, LANES), f32),
            pltpu.VMEM((n_cp, 1, tok), jnp.int32),
            pltpu.VMEM((n_tp - 1, tok, feat), bf16),
            pltpu.VMEM((n_tp - 1, tok, feat), bf16),
            dma((n_tp - 1, chunks)),
            dma((n_tp - 1, chunks)),
            dma(()),
            dma((3 + n_tp,)),
            dma((n_cp,)),
            dma((n_cp,)),
            dma((4, n_cp // 2 * chunks)),
            dma((n_cp * chunks,)),
            dma((n_tp - 1, n_tiles)),
            dma((n_tp - 1, n_tiles)),
            dma((n_tiles,)),
        ],
        compiler_params=pltpu.CompilerParams(
            collective_id=0, has_side_effects=True, vmem_limit_bytes=67_000_000
        ),
    )(
        hidden, norm_gain[None, :], w_query, w_key, w_value, w_out, cosine, sine,
        doc_ids[None, :], other_docs,
    )


def solution(mesh):
    in_specs = (
        P("cp", "tp"),
        P(),
        P(None, "tp"),
        P(None, "tp"),
        P(None, "tp"),
        P("tp", None),
        P("cp"),
    )
    body = functools.partial(shards, n_cp=mesh.shape["cp"], n_tp=mesh.shape["tp"])
    return jax.shard_map(
        body, mesh=mesh, in_specs=in_specs, out_specs=P("cp", "tp"), check_vma=False
    )
```

```python
import functools

import jax
import jax.numpy as jnp
from jax import lax
from jax.experimental import pallas as pl
from jax.experimental.pallas import tpu as pltpu
from jax.sharding import PartitionSpec as P

HEADS = 32
KV_HEADS = 8
HEAD_SIZE = 128
GROUP = HEADS // KV_HEADS

epsilon = 1e-05
rope_base = 500000.0
LOG2E = 1.4426950408889634
SCALE = HEAD_SIZE ** (-0.5) * LOG2E
FLOOR = -1e29
MASKED = -1e30
CHUNK = 128
QTILE = 128
NEAR = 9
LANES = 128
MESH = pl.DeviceIdType.MESH


def tables(positions):
    half = HEAD_SIZE // 2
    freqs = rope_base ** (-jnp.arange(half, dtype=jnp.float32) * 2.0 / HEAD_SIZE)
    angles = positions.astype(jnp.float32)[:, None] * freqs[None, :]
    cosine = jnp.cos(angles)
    sine = jnp.sin(angles)
    return (
        jnp.concatenate([cosine, cosine], axis=1),
        jnp.concatenate([-sine, sine], axis=1),
    )


def columns_of(n_cp):
    chips = n_cp // 2
    cols = 1
    while cols * cols * 4 <= chips:
        cols *= 2
    return cols


def layer_kernel(
    hid_hbm, gain_ref, wq_hbm, wk_hbm, wv_hbm, wo_hbm, cos_ref, sin_ref, docs_ref, qdoc_ref,
    out_hbm,
    hid, wq, kv, q, normed, docs, recv,
    hid_send, hid_recv, own_sem, w_sem, doc_send, doc_recv, kv_send, kv_recv,
    part_send, part_recv, out_sem,
    *, n_cp, n_tp, longest,
):
    tok, feat = hid_hbm.shape
    width = gain_ref.shape[1]
    q_cols = wq.shape[1]
    kv_cols = kv.shape[1]
    n_kv = kv_cols // (2 * HEAD_SIZE)
    chunks = tok // CHUNK
    n_tiles = tok // QTILE
    cols = columns_of(n_cp)
    rows_z = n_cp // (2 * cols)
    window = min((longest + tok - 2) // tok, n_cp - 1)
    chip_window = (window + 1) // 2
    near = min(NEAR, window + 1)

    me = lax.axis_index("cp")
    rank = lax.axis_index("tp")
    core = lax.rem(me, 2)
    my_x = lax.rem(me // 2, cols)
    my_z = me // (2 * cols)

    def peer_of(by):
        return lax.rem(rank + by, n_tp)

    barrier = pltpu.get_barrier_semaphore()
    for by in range(1, n_tp):
        pl.semaphore_signal(barrier, inc=1, device_id={"tp": peer_of(by)}, device_id_type=MESH)

    def greet(by, carry):
        pl.semaphore_signal(
            barrier, inc=1, device_id={"cp": lax.rem(me + by, n_cp)}, device_id_type=MESH
        )
        return carry

    lax.fori_loop(1, n_cp, greet, 0)

    own_copy = pltpu.make_async_copy(hid_hbm, hid.at[rank], own_sem)
    own_copy.start()
    docs[me] = docs_ref[...]
    wq_copy = pltpu.make_async_copy(wq_hbm, wq, w_sem.at[2])

    def hid_copy(by, t):
        rows = pl.ds(t * CHUNK, CHUNK)
        return pltpu.make_async_remote_copy(
            src_ref=hid_hbm.at[rows],
            dst_ref=hid.at[rank, rows],
            send_sem=hid_send.at[by - 1, t],
            recv_sem=hid_recv.at[n_tp - 1 - by, t],
            device_id={"tp": peer_of(by)},
            device_id_type=MESH,
        )

    def doc_copy(source, target):
        return pltpu.make_async_remote_copy(
            src_ref=docs_ref,
            dst_ref=docs.at[source],
            send_sem=doc_send.at[target],
            recv_sem=doc_recv.at[source],
            device_id={"cp": target},
            device_id_type=MESH,
        )

    last_target = jnp.minimum(me + window, n_cp - 1)

    def doc_start(target, carry):
        doc_copy(me, target).start()
        return carry

    def begin():
        pl.semaphore_wait(barrier, n_cp - 1 + n_tp - 1)
        for t in range(chunks):
            for by in range(1, n_tp):
                hid_copy(by, t).start()
        lax.fori_loop(me + 1, last_target + 1, doc_start, 0)

    def takes(z, x, zs, xs):
        reach = z * cols - (zs * cols + xs) <= chip_window
        by_z = (xs == x) & (zs < z) & reach
        from_left = (xs < x) & (zs <= z) & (z * cols + x - (zs * cols + xs) <= chip_window)
        from_right = (xs > x) & (zs < z) & reach
        return by_z | from_left | from_right

    def block_copy(direction, zs, xs, ks, t, target):
        chip = zs * cols + xs
        s = chip * 2 + ks
        rows = pl.ds(pl.multiple_of(s * tok + t * CHUNK, CHUNK), CHUNK)
        return pltpu.make_async_remote_copy(
            src_ref=kv.at[rows],
            dst_ref=kv.at[rows],
            send_sem=kv_send.at[direction, chip * chunks + t],
            recv_sem=kv_recv.at[s * chunks + t],
            device_id={"cp": target},
            device_id_type=MESH,
        )

    def hops(zs, xs):
        own_chip = (zs == my_z) & (xs == my_x)
        return (
            ((xs == my_x) & (my_z + 1 < rows_z) & takes(my_z + 1, my_x, zs, xs), me + 2 * cols),
            ((xs <= my_x) & (my_x + 1 < cols) & takes(my_z, my_x + 1, zs, xs), me + 2),
            ((xs >= my_x) & (my_x >= 1) & takes(my_z, my_x - 1, zs, xs), me - 2),
            (jnp.logical_not(own_chip) | (core == 0), me + 1 - 2 * core),
        )

    def forward(zs, xs, t):
        for direction, (wanted, target) in enumerate(hops(zs, xs)):
            @pl.when(wanted)
            def _():
                block_copy(direction, zs, xs, core, t, target).start()

    def arrive(zs, xs, ks, t, relay):
        in_range = (zs >= 0) & (xs >= 0) & (xs < cols) & (t >= 0) & (t < chunks)
        own_chip = (zs == my_z) & (xs == my_x)
        if relay:
            wanted = in_range & takes(my_z, my_x, zs, xs)
        else:
            wanted = in_range & (takes(my_z, my_x, zs, xs) | (own_chip & (core == 1)))

        @pl.when(wanted)
        def _():
            block_copy(0, zs, xs, ks, t, me).wait_recv()
            if relay:
                forward(zs, xs, t)

    stages = [[] for _ in range(chunks + (rows_z - 1) * chunks + 3)]
    settled = {0: chunks + 1}
    late = [
        (dz, group + 1 - dz)
        for group in range(chunks - 1, chunks + rows_z - 2)
        for dz in range(1, rows_z)
        if 0 <= group + 1 - dz < chunks
    ]
    for dz in range(rows_z):
        for t in range(chunks):
            if dz == 0:
                first = t
            elif (dz, t) in late:
                first = chunks + late.index((dz, t))
            else:
                first = t + dz - 1
            if dz:
                stages[first].append((0, dz, t))
            stages[first + 1].append((1, dz, t))
            stages[first + 2].append((2, dz, t))
            settled[dz] = max(settled.get(dz, 0), first + 2)
    while not stages[-1]:
        stages.pop()
    for stage_events in stages:
        stage_events.sort()

    def run_stage(k):
        for i, events in enumerate(stages):
            @pl.when(k == i)
            def _():
                for kind, dz, t in events:
                    if kind == 0:
                        arrive(my_z - dz, my_x, core, t, True)
                for dx in range(1, cols):
                    for kind, dz, t in events:
                        if kind == 1:
                            arrive(my_z - dz, my_x - dx, core, t, True)
                            arrive(my_z - dz, my_x + dx, core, t, True)
                for kind, dz, t in events:
                    if kind == 2:
                        def from_core(xs, carry):
                            own_chip = (dz == 0) & (xs == my_x)

                            @pl.when(jnp.logical_not(own_chip))
                            def _():
                                arrive(my_z - dz, xs, 1 - core, t, False)

                            return carry

                        lax.fori_loop(0, cols, from_core, 0)
                if i == chunks - 1:
                    for t in range(chunks):
                        arrive(my_z, my_x, 1 - core, t, False)

    def projections(wkv):
        wk_copy = pltpu.make_async_copy(wk_hbm, wkv.at[:, pl.ds(0, kv_cols // 2)], w_sem.at[0])
        wv_copy = pltpu.make_async_copy(
            wv_hbm, wkv.at[:, pl.ds(kv_cols // 2, kv_cols // 2)], w_sem.at[1]
        )
        wk_copy.start()
        wv_copy.start()
        wq_copy.start()
        begin()
        own_copy.wait()
        wk_copy.wait()
        wv_copy.wait()
        part_rows = 32

        def rope(raw, cosine, sine):
            turned = raw * cosine + pltpu.roll(raw, HEAD_SIZE // 2, 1) * sine
            return turned.astype(jnp.bfloat16)

        def chunk_step(t, carry):
            base = pl.multiple_of(t * CHUNK, CHUNK)
            for by in range(1, n_tp):
                pltpu.make_async_remote_copy(
                    src_ref=hid.at[peer_of(by), pl.ds(base, CHUNK)],
                    dst_ref=hid.at[peer_of(by), pl.ds(base, CHUNK)],
                    send_sem=hid_send.at[by - 1, t],
                    recv_sem=hid_recv.at[by - 1, t],
                    device_id={"tp": peer_of(by)},
                    device_id_type=MESH,
                ).wait_recv()

            def norm_part(i, carry):
                rows = pl.ds(pl.multiple_of(base + i * part_rows, part_rows), part_rows)
                total = jnp.zeros((part_rows, LANES), jnp.float32)
                for j in range(n_tp):
                    wide = hid[j, rows, :].astype(jnp.float32)
                    square = wide * wide
                    for c in range(feat // LANES):
                        total = total + square[:, c * LANES : (c + 1) * LANES]
                mean = jnp.sum(total, axis=1, keepdims=True) / width
                inverse_rms = lax.rsqrt(mean + epsilon)
                out_rows = pl.ds(pl.multiple_of(i * part_rows, part_rows), part_rows)
                for j in range(n_tp):
                    wide = hid[j, rows, :].astype(jnp.float32)
                    gain = gain_ref[:, j * feat : (j + 1) * feat]
                    normed[out_rows, j * feat : (j + 1) * feat] = (
                        wide * inverse_rms * gain
                    ).astype(jnp.bfloat16)
                return carry

            lax.fori_loop(0, CHUNK // part_rows, norm_part, 0)
            rows = pl.ds(base, CHUNK)
            cosine = cos_ref[rows, :]
            sine = sin_ref[rows, :]
            own_rows = pl.ds(pl.multiple_of(me * tok + t * CHUNK, CHUNK), CHUNK)
            for g in range(2 * n_kv):
                lanes = slice(g * HEAD_SIZE, (g + 1) * HEAD_SIZE)
                if g % 2 == 0:
                    pair = jnp.dot(
                        normed[...],
                        wkv[:, g * HEAD_SIZE : (g + 2) * HEAD_SIZE],
                        preferred_element_type=jnp.float32,
                    )
                raw = pair[:, (g % 2) * HEAD_SIZE : (g % 2 + 1) * HEAD_SIZE]
                kv[own_rows, lanes] = rope(raw, cosine, sine) if g < n_kv else raw.astype(jnp.bfloat16)

            @pl.when(t == 0)
            def _():
                wq_copy.wait()

            def query_group(g, carry):
                cut = pl.multiple_of(g * GROUP * HEAD_SIZE, HEAD_SIZE)
                raw = jnp.dot(
                    normed[...],
                    wq[:, pl.ds(cut, GROUP * HEAD_SIZE)],
                    preferred_element_type=jnp.float32,
                )
                for h in range(GROUP):
                    q[g * GROUP + h, rows, :] = rope(
                        raw[:, h * HEAD_SIZE : (h + 1) * HEAD_SIZE], cosine, sine
                    )
                return carry

            query_group(0, 0)
            forward(my_z, my_x, t)
            lax.fori_loop(1, n_kv, query_group, 0)
            run_stage(t)
            return carry

        lax.fori_loop(0, chunks, chunk_step, 0)

    pl.run_scoped(projections, pltpu.VMEM((width, kv_cols), jnp.bfloat16))

    wo_copies = [
        pltpu.make_async_copy(
            wo_hbm.at[:, pl.ds(j * feat, feat)], wq.at[pl.ds(j * q_cols, q_cols)], w_sem.at[3 + j]
        )
        for j in range(n_tp)
    ]
    for copy in wo_copies:
        copy.start()

    def attention(acc, best, denom, stage):
        strips = feat // LANES
        block_lanes = tok // LANES
        def doc_strip(s):
            return s // strips, pl.ds(pl.multiple_of(lax.rem(s, strips) * LANES, LANES), LANES)

        def key_docs(s):
            row = jnp.broadcast_to(docs[s], (LANES, tok))
            number = lax.broadcasted_iota(jnp.int32, (LANES, tok), 0)
            one_hot = jnp.where(row == number, 1.0, 0.0).astype(jnp.float32)
            j, lanes = doc_strip(s)
            hid[j, :, lanes] = one_hot.T.astype(jnp.bfloat16)

        def attend(g, start, size, blocks, first=False):
            count = len(blocks)
            key_rows = pl.ds(pl.multiple_of(blocks[0] * tok, tok), count * tok)
            key_lanes = pl.ds(pl.multiple_of(g * HEAD_SIZE, HEAD_SIZE), HEAD_SIZE)
            value_lanes = pl.ds(pl.multiple_of((n_kv + g) * HEAD_SIZE, HEAD_SIZE), HEAD_SIZE)
            numbers = []
            for s in blocks:
                j, lanes = doc_strip(s)
                numbers.append(hid[j, :, lanes])
            numbers = numbers[0] if count == 1 else jnp.concatenate(numbers, axis=0)
            keys = jnp.concatenate([kv[key_rows, key_lanes], numbers], axis=1)
            rows = pl.ds(start, size)
            heads = pl.ds(g * GROUP, GROUP)
            stacked = GROUP * size
            others = jnp.concatenate([qdoc_ref[rows, :]] * GROUP, axis=0)
            queries = jnp.concatenate(
                [q[heads, rows, :].reshape(stacked, HEAD_SIZE), others], axis=1
            )
            scores = lax.dot_general(
                queries, keys, (((1,), (1,)), ((), ())), preferred_element_type=jnp.float32
            )
            pieces = [
                scores[:, c * LANES : (c + 1) * LANES] * SCALE for c in range(count * block_lanes)
            ]
            if first:
                row = lax.broadcasted_iota(jnp.int32, (stacked, LANES), 0) % size
                lane = lax.broadcasted_iota(jnp.int32, (stacked, LANES), 1)
                pieces = [
                    jnp.where(row >= lane + c * LANES, p, MASKED) for c, p in enumerate(pieces)
                ]
            top = jnp.max(functools.reduce(jnp.maximum, pieces), axis=1, keepdims=True)
            shape = (GROUP, size, LANES)
            if first:
                new = jnp.broadcast_to(jnp.maximum(top, FLOOR), (stacked, LANES))
            else:
                old = best[heads, rows, :].reshape(stacked, LANES)
                new = jnp.maximum(old, top)
                correction = jnp.exp2(old - new)
            weights = [jnp.exp2(p - new) for p in pieces]
            total = functools.reduce(jnp.add, weights)
            rounded = jnp.concatenate([w.astype(jnp.bfloat16) for w in weights], axis=1)
            sums = jnp.dot(rounded, kv[key_rows, value_lanes], preferred_element_type=jnp.float32)
            if not first:
                total = denom[heads, rows, :].reshape(stacked, LANES) * correction + total
                sums = acc[heads, rows, :].reshape(stacked, LANES) * correction + sums
            best[heads, rows, :] = new.reshape(shape)
            denom[heads, rows, :] = total.reshape(shape)
            acc[heads, rows, :] = sums.reshape(shape)

        def all_tiles(s, first):
            def one(g, carry):
                attend(g, 0, tok, [s], first)
                return carry

            lax.fori_loop(0, n_kv, one, 0)

        key_docs(me)
        all_tiles(me, True)

        in_row = lax.rem(me, 2 * cols) + 1
        last_stage = len(stages) - 1

        def stages_before(o):
            distance = jnp.where(o < in_row, 0, (o - in_row) // (2 * cols) + 1)
            needed = jnp.where((o == 1) & (core == 1), chunks - 1, settled[0])
            for dz in range(1, rows_z):
                needed = jnp.where(distance >= dz, settled[dz], needed)
            return jnp.clip(jnp.maximum(chunks - 1 + o, needed), chunks - 1, last_stage)

        def take_stages(begin, end):
            def one(k, carry):
                run_stage(k)
                return carry

            lax.fori_loop(begin, end, one, 0)

        def docs_for(s):
            doc_copy(s, me).wait_recv()
            key_docs(s)

        def near_step(o, carry):
            take_stages(
                jnp.where(o == 1, chunks, stages_before(o - 1) + 1), stages_before(o) + 1
            )
            s = me - o

            @pl.when(s >= 0)
            def _():
                docs_for(s)
                all_tiles(s, False)

            return carry

        lax.fori_loop(1, near, near_step, 0)
        take_stages(stages_before(near - 1) + 1, last_stage + 1)

        def far_docs(o, carry):
            @pl.when(me - o >= 0)
            def _():
                docs_for(me - o)

            return carry

        lax.fori_loop(near, window + 1, far_docs, 0)
        for copy in wo_copies:
            copy.wait()

        n_far = jnp.maximum(jnp.minimum(window, me) + 1 - near, 0)
        col_step = min(512, feat)

        def part_copy(by, tile):
            rows = pl.ds(pl.multiple_of(tile * QTILE, QTILE), QTILE)
            return pltpu.make_async_remote_copy(
                src_ref=stage.at[by - 1, rows],
                dst_ref=recv.at[n_tp - 1 - by, rows],
                send_sem=part_send.at[by - 1, tile],
                recv_sem=part_recv.at[n_tp - 1 - by, tile],
                device_id={"tp": peer_of(by)},
                device_id_type=MESH,
            )

        def tile_step(tile, carry):
            rows = pl.ds(pl.multiple_of(tile * QTILE, QTILE), QTILE)

            start = pl.multiple_of(tile * QTILE, QTILE)

            def far_pair(i, carry):
                s = me - near - 1 - 2 * (i // n_kv)
                attend(lax.rem(i, n_kv), start, QTILE, [s, s + 1])
                return carry

            lax.fori_loop(0, n_far // 2 * n_kv, far_pair, 0)

            def far_last(g, carry):
                attend(g, start, QTILE, [me - near - n_far + 1])
                return carry

            lax.fori_loop(0, lax.rem(n_far, 2) * n_kv, far_last, 0)

            def finish(head, carry):
                total = jnp.sum(denom[head, rows, :], axis=1, keepdims=True)
                lanes = pl.ds(pl.multiple_of(head * HEAD_SIZE, HEAD_SIZE), HEAD_SIZE)
                normed[:, lanes] = (acc[head, rows, :] / total).astype(jnp.bfloat16)
                return carry

            lax.fori_loop(0, n_kv * GROUP, finish, 0)
            attended = normed[:, :q_cols]
            for by in list(range(1, n_tp)) + [0]:
                piece = pl.ds(pl.multiple_of(peer_of(by) * q_cols, q_cols), q_cols)
                for c in range(feat // col_step):
                    part = jnp.dot(
                        attended,
                        wq[piece, c * col_step : (c + 1) * col_step],
                        preferred_element_type=jnp.float32,
                    ).astype(jnp.bfloat16)
                    if by:
                        stage[by - 1, rows, c * col_step : (c + 1) * col_step] = part
                    else:
                        for h in range(col_step // LANES):
                            q[c * (col_step // LANES) + h, rows, :] = part[
                                :, h * LANES : (h + 1) * LANES
                            ]
            for by in range(1, n_tp):
                part_copy(by, tile).start()
            return carry

        lax.fori_loop(0, n_tiles, tile_step, 0)

        def out_copy(tile):
            rows = pl.ds(pl.multiple_of(tile * QTILE, QTILE), QTILE)
            return pltpu.make_async_copy(recv.at[0, rows], out_hbm.at[rows], out_sem.at[tile])

        def sum_step(tile, carry):
            rows = pl.ds(pl.multiple_of(tile * QTILE, QTILE), QTILE)
            for by in range(1, n_tp):
                part_copy(by, tile).wait_recv()
            for c in range(feat // LANES):
                lanes = slice(c * LANES, (c + 1) * LANES)
                total = q[c, rows, :].astype(jnp.float32)
                for by in range(1, n_tp):
                    total = total + recv[by - 1, rows, lanes].astype(jnp.float32)
                recv[0, rows, lanes] = total.astype(jnp.bfloat16)
            out_copy(tile).start()
            return carry

        lax.fori_loop(0, n_tiles, sum_step, 0)

        def end_step(tile, carry):
            for by in range(1, n_tp):
                part_copy(by, tile).wait_send()
            out_copy(tile).wait()
            return carry

        lax.fori_loop(0, n_tiles, end_step, 0)

    state = pltpu.VMEM(q.shape, jnp.float32)
    pl.run_scoped(
        attention, state, state, state, pltpu.VMEM((n_tp - 1, tok, feat), jnp.bfloat16)
    )

    def sent_step(i, carry):
        t = lax.rem(i, chunks)
        chip = i // chunks
        zs, xs = chip // cols, lax.rem(chip, cols)
        own_chip = (zs == my_z) & (xs == my_x)
        held = own_chip | ((zs <= my_z) & takes(my_z, my_x, zs, xs))
        for direction, (wanted, target) in enumerate(hops(zs, xs)):
            @pl.when(held & wanted)
            def _():
                block_copy(direction, zs, xs, core, t, target).wait_send()

        return carry

    lax.fori_loop(0, n_cp // 2 * chunks, sent_step, 0)

    def doc_sent(target, carry):
        doc_copy(me, target).wait_send()
        return carry

    lax.fori_loop(me + 1, last_target + 1, doc_sent, 0)
    for t in range(chunks):
        for by in range(1, n_tp):
            hid_copy(by, t).wait_send()


def shards(hidden, norm_gain, w_query, w_key, w_value, w_out, doc_ids, *, n_cp, n_tp):
    tok, feat = hidden.shape
    width = norm_gain.shape[0]
    q_cols = w_query.shape[1]
    kv_cols = 2 * w_key.shape[1]
    seq = tok * n_cp
    longest = seq * 3 // 4
    chunks = tok // CHUNK
    n_tiles = tok // QTILE
    cp_rank = lax.axis_index("cp")
    positions = cp_rank * tok + jnp.arange(tok, dtype=jnp.int32)
    cosine, sine = tables(positions)
    number = jnp.arange(LANES, dtype=jnp.int32)
    other_docs = jnp.where(doc_ids[:, None] == number[None, :], 0.0, MASKED).astype(jnp.bfloat16)
    vmem = pl.BlockSpec(memory_space=pltpu.VMEM)
    hbm = pl.BlockSpec(memory_space=pl.ANY)
    bf16 = jnp.bfloat16
    dma = pltpu.SemaphoreType.DMA
    heads = q_cols // HEAD_SIZE
    return pl.pallas_call(
        functools.partial(layer_kernel, n_cp=n_cp, n_tp=n_tp, longest=longest),
        out_shape=jax.ShapeDtypeStruct((tok, feat), bf16),
        in_specs=[hbm, vmem, hbm, hbm, hbm, hbm, vmem, vmem, vmem, vmem],
        out_specs=hbm,
        scratch_shapes=[
            pltpu.VMEM((n_tp, tok, feat), bf16),
            pltpu.VMEM((width, q_cols), bf16),
            pltpu.VMEM((seq, kv_cols), bf16),
            pltpu.VMEM((heads, tok, HEAD_SIZE), bf16),
            pltpu.VMEM((CHUNK, width), bf16),
            pltpu.VMEM((n_cp, 1, tok), jnp.int32),
            pltpu.VMEM((n_tp - 1, tok, feat), bf16),
            dma((n_tp - 1, chunks)),
            dma((n_tp - 1, chunks)),
            dma(()),
            dma((3 + n_tp,)),
            dma((n_cp,)),
            dma((n_cp,)),
            dma((4, n_cp // 2 * chunks)),
            dma((n_cp * chunks,)),
            dma((n_tp - 1, n_tiles)),
            dma((n_tp - 1, n_tiles)),
            dma((n_tiles,)),
        ],
        compiler_params=pltpu.CompilerParams(
            collective_id=0, has_side_effects=True, vmem_limit_bytes=67_000_000
        ),
    )(
        hidden, norm_gain[None, :], w_query, w_key, w_value, w_out, cosine, sine,
        doc_ids[None, :], other_docs,
    )


def solution(mesh):
    in_specs = (
        P("cp", "tp"),
        P(),
        P(None, "tp"),
        P(None, "tp"),
        P(None, "tp"),
        P("tp", None),
        P("cp"),
    )
    body = functools.partial(shards, n_cp=mesh.shape["cp"], n_tp=mesh.shape["tp"])
    return jax.shard_map(
        body, mesh=mesh, in_specs=in_specs, out_specs=P("cp", "tp"), check_vma=False
    )
```

```python
import functools

import jax
import jax.numpy as jnp
from jax import lax
from jax.experimental import pallas as pl
from jax.experimental.pallas import tpu as pltpu
from jax.sharding import PartitionSpec as P

HEADS = 32
KV_HEADS = 8
HEAD_SIZE = 128
GROUP = HEADS // KV_HEADS

epsilon = 1e-05
rope_base = 500000.0
LOG2E = 1.4426950408889634
SCALE = HEAD_SIZE ** (-0.5) * LOG2E
FLOOR = -1e29
MASKED = -1e30
CHUNK = 128
QTILE = 128
LANES = 128
MESH = pl.DeviceIdType.MESH


def tables(positions):
    half = HEAD_SIZE // 2
    freqs = rope_base ** (-jnp.arange(half, dtype=jnp.float32) * 2.0 / HEAD_SIZE)
    angles = positions.astype(jnp.float32)[:, None] * freqs[None, :]
    cosine = jnp.cos(angles)
    sine = jnp.sin(angles)
    return (
        jnp.concatenate([cosine, cosine], axis=1),
        jnp.concatenate([-sine, sine], axis=1),
    )


def columns_of(n_cp):
    chips = n_cp // 2
    cols = 1
    while cols * cols * 4 <= chips:
        cols *= 2
    return cols


def layer_kernel(
    hid_hbm, gain_hbm, wq_hbm, wk_hbm, wv_hbm, wo_hbm, cos_ref, sin_ref, docs_hbm,
    own_hbm, got_hbm,
    hid, wq, kv, q, normed, docs, qdoc, gain, mine,
    hid_send, hid_recv, own_sem, small_sem, w_sem, doc_send, doc_recv, kv_send, kv_recv,
    part_send, part_recv, out_sem,
    *, n_cp, n_tp, longest,
):
    tok, feat = hid_hbm.shape
    width = gain_hbm.shape[0]
    q_cols = wq.shape[1]
    kv_cols = kv.shape[1]
    n_kv = kv_cols // (2 * HEAD_SIZE)
    chunks = tok // CHUNK
    n_tiles = tok // QTILE
    cols = columns_of(n_cp)
    rows_z = n_cp // (2 * cols)
    window = min((longest + tok - 2) // tok, n_cp - 1)
    chip_window = (window + 1) // 2
    pairs = (window + 1) // 2
    half = tok // 2

    me = lax.axis_index("cp")
    rank = lax.axis_index("tp")
    core = lax.rem(me, 2)
    my_x = lax.rem(me // 2, cols)
    my_z = me // (2 * cols)

    def peer_of(by):
        return lax.rem(rank + by, n_tp)

    barrier = pltpu.get_barrier_semaphore()
    for by in range(1, n_tp):
        pl.semaphore_signal(barrier, inc=1, device_id={"tp": peer_of(by)}, device_id_type=MESH)

    def greet(by, carry):
        pl.semaphore_signal(
            barrier, inc=1, device_id={"cp": lax.rem(me + by, n_cp)}, device_id_type=MESH
        )
        return carry

    lax.fori_loop(1, n_cp, greet, 0)

    own_copy = pltpu.make_async_copy(hid_hbm, hid.at[rank], own_sem)
    own_copy.start()
    gain_copy = pltpu.make_async_copy(gain_hbm, gain.at[0], small_sem.at[0])
    docs_copy = pltpu.make_async_copy(docs_hbm, docs.at[me, 0], small_sem.at[1])
    gain_copy.start()
    docs_copy.start()
    wq_copy = pltpu.make_async_copy(wq_hbm, wq, w_sem.at[2])

    def hid_copy(by, t):
        rows = pl.ds(t * CHUNK, CHUNK)
        return pltpu.make_async_remote_copy(
            src_ref=hid_hbm.at[rows],
            dst_ref=hid.at[rank, rows],
            send_sem=hid_send.at[by - 1, t],
            recv_sem=hid_recv.at[n_tp - 1 - by, t],
            device_id={"tp": peer_of(by)},
            device_id_type=MESH,
        )

    def doc_copy(source, target):
        return pltpu.make_async_remote_copy(
            src_ref=docs.at[source],
            dst_ref=docs.at[source],
            send_sem=doc_send.at[target],
            recv_sem=doc_recv.at[source],
            device_id={"cp": target},
            device_id_type=MESH,
        )

    last_target = jnp.minimum(me + window, n_cp - 1)

    def doc_start(target, carry):
        doc_copy(me, target).start()
        return carry

    def begin():
        pl.semaphore_wait(barrier, n_cp - 1 + n_tp - 1)
        for t in range(chunks):
            for by in range(1, n_tp):
                hid_copy(by, t).start()
        docs_copy.wait()
        lax.fori_loop(me + 1, last_target + 1, doc_start, 0)
        gain_copy.wait()

    def takes(z, x, zs, xs):
        reach = z * cols - (zs * cols + xs) <= chip_window
        by_z = (xs == x) & (zs < z) & reach
        from_left = (xs < x) & (zs <= z) & (z * cols + x - (zs * cols + xs) <= chip_window)
        from_right = (xs > x) & (zs < z) & reach
        return by_z | from_left | from_right

    def block_copy(direction, zs, xs, ks, t, target):
        chip = zs * cols + xs
        s = chip * 2 + ks
        rows = pl.ds(pl.multiple_of(s * tok + t * CHUNK, CHUNK), CHUNK)
        return pltpu.make_async_remote_copy(
            src_ref=kv.at[rows],
            dst_ref=kv.at[rows],
            send_sem=kv_send.at[direction, chip * chunks + t],
            recv_sem=kv_recv.at[s * chunks + t],
            device_id={"cp": target},
            device_id_type=MESH,
        )

    def hops(zs, xs):
        own_chip = (zs == my_z) & (xs == my_x)
        return (
            ((xs == my_x) & (my_z + 1 < rows_z) & takes(my_z + 1, my_x, zs, xs), me + 2 * cols),
            ((xs <= my_x) & (my_x + 1 < cols) & takes(my_z, my_x + 1, zs, xs), me + 2),
            ((xs >= my_x) & (my_x >= 1) & takes(my_z, my_x - 1, zs, xs), me - 2),
            (jnp.logical_not(own_chip) | (core == 0), me + 1 - 2 * core),
        )

    def forward(zs, xs, t):
        for direction, (wanted, target) in enumerate(hops(zs, xs)):
            @pl.when(wanted)
            def _():
                block_copy(direction, zs, xs, core, t, target).start()

    def arrive(zs, xs, ks, t, relay):
        in_range = (zs >= 0) & (xs >= 0) & (xs < cols) & (t >= 0) & (t < chunks)
        own_chip = (zs == my_z) & (xs == my_x)
        if relay:
            wanted = in_range & takes(my_z, my_x, zs, xs)
        else:
            wanted = in_range & (takes(my_z, my_x, zs, xs) | (own_chip & (core == 1)))

        @pl.when(wanted)
        def _():
            block_copy(0, zs, xs, ks, t, me).wait_recv()
            if relay:
                forward(zs, xs, t)

    along = {}
    for dz in range(1, rows_z):
        for t in range(chunks):
            group = dz + t - 1
            if group == 0 or (group < chunks - 1 and (dz > 1 or group < chunks - 2)):
                along[dz, t] = group
            elif group == chunks - 2:
                along[dz, t] = chunks - 1
    late = sorted(
        (dz + t, t if t == chunks - 1 and dz == 1 else 0, dz, t)
        for dz in range(1, rows_z)
        for t in range(chunks)
        if (dz, t) not in along
    )
    late = [(dz, t) for _, _, dz, t in late]
    for i, event in enumerate(late):
        along[event] = chunks + 1 + 2 * i

    def later(stage, busy, calm):
        return stage + (calm if stage < chunks - 1 else busy)

    stages = [[] for _ in range(3 * chunks + 2 * len(late) + 16)]
    settled = {}
    for dz in range(rows_z):
        for t in range(chunks):
            first = along[dz, t] if dz else t
            if dz:
                stages[first].append((0, dz, t))
            by_x = later(first, 3, 1)
            stages[by_x].append((1, dz, t))
            stages[by_x + 1].append((2, dz, t))
            if t < chunks // 2:
                settled[dz] = max(settled.get(dz, 0), by_x + 1)
    for dz in range(1, rows_z):
        settled[dz] = max(settled[dz], settled[dz - 1])
    while not stages[-1]:
        stages.pop()

    def run_stage(k):
        for i, events in enumerate(stages):
            @pl.when(k == i)
            def _():
                for kind, dz, t in events:
                    if kind == 0:
                        arrive(my_z - dz, my_x, core, t, True)
                for dx in range(1, cols):
                    for kind, dz, t in events:
                        if kind == 1:
                            arrive(my_z - dz, my_x - dx, core, t, True)
                            arrive(my_z - dz, my_x + dx, core, t, True)
                for kind, dz, t in events:
                    if kind == 2:
                        def from_core(xs, carry):
                            own_chip = (dz == 0) & (xs == my_x)

                            @pl.when(jnp.logical_not(own_chip))
                            def _():
                                arrive(my_z - dz, xs, 1 - core, t, False)

                            return carry

                        lax.fori_loop(0, cols, from_core, 0)
                if i == chunks - 1:
                    for t in range(chunks):
                        arrive(my_z, my_x, 1 - core, t, False)

    def projections(wkv):
        wk_copy = pltpu.make_async_copy(wk_hbm, wkv.at[:, pl.ds(0, kv_cols // 2)], w_sem.at[0])
        wv_copy = pltpu.make_async_copy(
            wv_hbm, wkv.at[:, pl.ds(kv_cols // 2, kv_cols // 2)], w_sem.at[1]
        )
        wk_copy.start()
        wv_copy.start()
        wq_copy.start()
        begin()
        own_copy.wait()
        wk_copy.wait()
        wv_copy.wait()
        part_rows = 32

        def rope(raw, cosine, sine):
            turned = raw * cosine + pltpu.roll(raw, HEAD_SIZE // 2, 1) * sine
            return turned

        def chunk_step(t, carry):
            base = pl.multiple_of(t * CHUNK, CHUNK)
            for by in range(1, n_tp):
                pltpu.make_async_remote_copy(
                    src_ref=hid.at[peer_of(by), pl.ds(base, CHUNK)],
                    dst_ref=hid.at[peer_of(by), pl.ds(base, CHUNK)],
                    send_sem=hid_send.at[by - 1, t],
                    recv_sem=hid_recv.at[by - 1, t],
                    device_id={"tp": peer_of(by)},
                    device_id_type=MESH,
                ).wait_recv()

            def norm_part(i, carry):
                rows = pl.ds(pl.multiple_of(base + i * part_rows, part_rows), part_rows)
                total = jnp.zeros((part_rows, LANES), jnp.float32)
                for j in range(n_tp):
                    wide = hid[j, rows, :].astype(jnp.float32)
                    square = wide * wide
                    for c in range(feat // LANES):
                        total = total + square[:, c * LANES : (c + 1) * LANES]
                mean = jnp.sum(total, axis=1, keepdims=True) / width
                inverse_rms = lax.rsqrt(mean + epsilon)
                out_rows = pl.ds(pl.multiple_of(i * part_rows, part_rows), part_rows)
                for j in range(n_tp):
                    wide = hid[j, rows, :].astype(jnp.float32)
                    scale = gain[:, j * feat : (j + 1) * feat]
                    normed[out_rows, j * feat : (j + 1) * feat] = (
                        wide * inverse_rms * scale
                    ).astype(jnp.bfloat16)
                return carry

            lax.fori_loop(0, CHUNK // part_rows, norm_part, 0)
            rows = pl.ds(base, CHUNK)
            cosine = cos_ref[rows, :]
            sine = sin_ref[rows, :]
            own_rows = pl.ds(pl.multiple_of(me * tok + t * CHUNK, CHUNK), CHUNK)
            for g in range(2 * n_kv):
                lanes = slice(g * HEAD_SIZE, (g + 1) * HEAD_SIZE)
                if g % 2 == 0:
                    pair = jnp.dot(
                        normed[...],
                        wkv[:, g * HEAD_SIZE : (g + 2) * HEAD_SIZE],
                        preferred_element_type=jnp.float32,
                    )
                raw = pair[:, (g % 2) * HEAD_SIZE : (g % 2 + 1) * HEAD_SIZE]
                turned = rope(raw, cosine, sine) if g < n_kv else raw
                kv[own_rows, lanes] = turned.astype(jnp.bfloat16)

            @pl.when(t == 0)
            def _():
                wq_copy.wait()

            def query_group(g, carry):
                cut = pl.multiple_of(g * GROUP * HEAD_SIZE, HEAD_SIZE)
                raw = jnp.dot(
                    normed[...],
                    wq[:, pl.ds(cut, GROUP * HEAD_SIZE)],
                    preferred_element_type=jnp.float32,
                )
                for h in range(GROUP):
                    turned = rope(raw[:, h * HEAD_SIZE : (h + 1) * HEAD_SIZE], cosine, sine)
                    q[g * GROUP + h, rows, :] = (turned * SCALE).astype(jnp.bfloat16)
                return carry

            query_group(0, 0)
            forward(my_z, my_x, t)
            lax.fori_loop(1, n_kv, query_group, 0)
            run_stage(t)
            return carry

        lax.fori_loop(0, chunks, chunk_step, 0)

    pl.run_scoped(projections, pltpu.VMEM((width, kv_cols), jnp.bfloat16))

    wo_copies = [
        pltpu.make_async_copy(
            wo_hbm.at[:, pl.ds(j * feat, feat)], wq.at[pl.ds(j * q_cols, q_cols)], w_sem.at[3 + j]
        )
        for j in range(n_tp)
    ]
    for copy in wo_copies:
        copy.start()

    def attention(acc, best, denom, stage):
        strips = feat // LANES
        def doc_strip(s):
            return s // strips, pl.ds(pl.multiple_of(lax.rem(s, strips) * LANES, LANES), LANES)

        def docs_columns(s, other, same):
            row = jnp.broadcast_to(docs[s], (LANES, tok))
            number = lax.broadcasted_iota(jnp.int32, (LANES, tok), 0)
            return jnp.where(row == number, same, other).astype(jnp.float32).T.astype(jnp.bfloat16)

        def key_docs(s):
            j, lanes = doc_strip(s)
            hid[j, :, lanes] = docs_columns(s, 0.0, 1.0)

        def attend(g, start, size, segments, first=False):
            key_lanes = pl.ds(pl.multiple_of(g * HEAD_SIZE, HEAD_SIZE), HEAD_SIZE)
            value_lanes = pl.ds(pl.multiple_of((n_kv + g) * HEAD_SIZE, HEAD_SIZE), HEAD_SIZE)
            keys, values = [], []
            for block, begin, length in segments:
                present = (block >= 0) & (me - block <= window)
                block = jnp.where(present, block, me)
                j, lanes = doc_strip(block)
                numbers = hid[j, begin : begin + length, lanes]
                if not first:
                    numbers = jnp.where(present, numbers, jnp.ones_like(numbers))
                key_rows = pl.ds(pl.multiple_of(block * tok + begin, length), length)
                keys.append(jnp.concatenate([kv[key_rows, key_lanes], numbers], axis=1))
                values.append(kv[key_rows, value_lanes])
            keys = jnp.concatenate(keys, axis=0)
            values = jnp.concatenate(values, axis=0)
            key_count = keys.shape[0]
            rows = pl.ds(start, size)
            heads = pl.ds(g * GROUP, GROUP)
            stacked = GROUP * size
            others = jnp.concatenate([qdoc[rows, :]] * GROUP, axis=0)
            queries = jnp.concatenate(
                [q[heads, rows, :].reshape(stacked, HEAD_SIZE), others], axis=1
            )
            scores = lax.dot_general(
                queries, keys, (((1,), (1,)), ((), ())), preferred_element_type=jnp.float32
            )
            pieces = [
                scores[:, c * LANES : (c + 1) * LANES] for c in range(key_count // LANES)
            ]
            if first:
                row = lax.broadcasted_iota(jnp.int32, (stacked, LANES), 0) % size
                lane = lax.broadcasted_iota(jnp.int32, (stacked, LANES), 1)
                pieces = [
                    jnp.where(row >= lane + c * LANES, p, MASKED) for c, p in enumerate(pieces)
                ]
            top = jnp.max(functools.reduce(jnp.maximum, pieces), axis=1, keepdims=True)
            shape = (GROUP, size, LANES)
            if first:
                new = jnp.broadcast_to(jnp.maximum(top, FLOOR), (stacked, LANES))
            else:
                old = best[heads, rows, :].reshape(stacked, LANES)
                new = jnp.maximum(old, top)
                correction = jnp.exp2(old - new)
            weights = [jnp.exp2(p - new) for p in pieces]
            total = functools.reduce(jnp.add, weights)
            rounded = jnp.concatenate([w.astype(jnp.bfloat16) for w in weights], axis=1)
            sums = jnp.dot(rounded, values, preferred_element_type=jnp.float32)
            if not first:
                total = denom[heads, rows, :].reshape(stacked, LANES) * correction + total
                sums = acc[heads, rows, :].reshape(stacked, LANES) * correction + sums
            best[heads, rows, :] = new.reshape(shape)
            denom[heads, rows, :] = total.reshape(shape)
            acc[heads, rows, :] = sums.reshape(shape)

        def groups(begin, end, segments, first=False):
            def one(g, carry):
                attend(g, 0, tok, segments, first)
                return carry

            lax.fori_loop(begin, end, one, 0)


        in_row = lax.rem(me, 2 * cols) + 1
        last_stage = len(stages) - 1

        def stages_by(p):
            o = 2 * (p // 2)
            distance = jnp.where(o < in_row, 0, (o - in_row) // (2 * cols) + 1)
            needed = jnp.where(o == 0, 0, settled[0])
            for dz in range(1, rows_z):
                needed = jnp.where((distance >= dz) & (o > 0), settled[dz], needed)
            return jnp.clip(jnp.maximum(chunks - 1 + p, needed), chunks - 1, last_stage)

        def take_stages(begin, end):
            def one(k, carry):
                run_stage(k)
                return carry

            lax.fori_loop(begin, end, one, 0)

        def docs_for(s):
            doc_copy(s, me).wait_recv()
            key_docs(s)

        key_docs(me)
        own_docs = docs_columns(me, MASKED, 0.0)
        qdoc[...] = own_docs
        groups(0, n_kv // 2, [(me, 0, tok)], True)
        take_stages(chunks, stages_by(1) + 1)
        groups(n_kv // 2, n_kv, [(me, 0, tok)], True)

        def near_step(i, carry):
            take_stages(stages_by(2 * i - 1) + 1, stages_by(2 * i) + 1)
            last = me - 2 * i
            segments = [(last, 0, half), (last + 1, 0, half)]

            @pl.when(last + 1 >= 0)
            def _():
                docs_for(last + 1)

            @pl.when((last >= 0) & (2 * i <= window))
            def _():
                docs_for(last)

            @pl.when(last + 1 >= 0)
            def _():
                groups(0, n_kv // 2, segments)

            take_stages(stages_by(2 * i) + 1, stages_by(2 * i + 1) + 1)

            @pl.when(last + 1 >= 0)
            def _():
                groups(n_kv // 2, n_kv, segments)

            return carry

        lax.fori_loop(1, pairs + 1, near_step, 0)
        take_stages(stages_by(2 * pairs + 1) + 1, last_stage + 1)
        for copy in wo_copies:
            copy.wait()

        n_far = (jnp.minimum(window, me) + 3) // 4
        col_step = min(512, feat)

        def part_copy(by, tile):
            rows = pl.ds(pl.multiple_of(tile * QTILE, QTILE), QTILE)
            return pltpu.make_async_remote_copy(
                src_ref=stage.at[by - 1, rows],
                dst_ref=got_hbm.at[n_tp - 1 - by, rows],
                send_sem=part_send.at[by - 1, tile],
                recv_sem=part_recv.at[n_tp - 1 - by, tile],
                device_id={"tp": peer_of(by)},
                device_id_type=MESH,
            )

        def mine_copy(tile):
            rows = pl.ds(pl.multiple_of(tile * QTILE, QTILE), QTILE)
            return pltpu.make_async_copy(mine.at[rows], own_hbm.at[rows], out_sem.at[tile])

        def tile_step(tile, carry):
            rows = pl.ds(pl.multiple_of(tile * QTILE, QTILE), QTILE)

            start = pl.multiple_of(tile * QTILE, QTILE)

            def far_step(i, carry):
                last = me - 4 * (i // n_kv) - 4
                segments = [(last + n, half, half) for n in range(4)]
                attend(lax.rem(i, n_kv), start, QTILE, segments)
                return carry

            lax.fori_loop(0, n_far * n_kv, far_step, 0)

            def finish(head, carry):
                total = jnp.sum(denom[head, rows, :], axis=1, keepdims=True)
                lanes = pl.ds(pl.multiple_of(head * HEAD_SIZE, HEAD_SIZE), HEAD_SIZE)
                normed[:, lanes] = (acc[head, rows, :] / total).astype(jnp.bfloat16)
                return carry

            lax.fori_loop(0, n_kv * GROUP, finish, 0)
            attended = normed[:, :q_cols]
            for by in list(range(1, n_tp)) + [0]:
                piece = pl.ds(pl.multiple_of(peer_of(by) * q_cols, q_cols), q_cols)
                target = stage.at[by - 1] if by else mine
                for c in range(feat // col_step):
                    cut = slice(c * col_step, (c + 1) * col_step)
                    target[rows, cut] = jnp.dot(
                        attended, wq[piece, cut], preferred_element_type=jnp.float32
                    ).astype(jnp.bfloat16)
                    if c == 0 and by != 1 % n_tp:
                        part_copy((by or n_tp) - 1, tile).start()
            mine_copy(tile).start()
            return carry

        lax.fori_loop(0, n_tiles, tile_step, 0)

        def end_step(tile, carry):
            for by in range(1, n_tp):
                part_copy(by, tile).wait_recv()
                part_copy(by, tile).wait_send()
            mine_copy(tile).wait()
            return carry

        lax.fori_loop(0, n_tiles, end_step, 0)

    state = pltpu.VMEM(q.shape, jnp.float32)
    pl.run_scoped(
        attention, state, state, state, pltpu.VMEM((n_tp - 1, tok, feat), jnp.bfloat16)
    )

    def sent_step(i, carry):
        t = lax.rem(i, chunks)
        chip = i // chunks
        zs, xs = chip // cols, lax.rem(chip, cols)
        own_chip = (zs == my_z) & (xs == my_x)
        held = own_chip | ((zs <= my_z) & takes(my_z, my_x, zs, xs))
        for direction, (wanted, target) in enumerate(hops(zs, xs)):
            @pl.when(held & wanted)
            def _():
                block_copy(direction, zs, xs, core, t, target).wait_send()

        return carry

    lax.fori_loop(0, n_cp // 2 * chunks, sent_step, 0)

    def doc_sent(target, carry):
        doc_copy(me, target).wait_send()
        return carry

    lax.fori_loop(me + 1, last_target + 1, doc_sent, 0)
    for t in range(chunks):
        for by in range(1, n_tp):
            hid_copy(by, t).wait_send()


def shards(hidden, norm_gain, w_query, w_key, w_value, w_out, doc_ids, *, n_cp, n_tp):
    tok, feat = hidden.shape
    width = norm_gain.shape[0]
    q_cols = w_query.shape[1]
    kv_cols = 2 * w_key.shape[1]
    seq = tok * n_cp
    longest = seq * 3 // 4
    chunks = tok // CHUNK
    n_tiles = tok // QTILE
    cp_rank = lax.axis_index("cp")
    positions = cp_rank * tok + jnp.arange(tok, dtype=jnp.int32)
    cosine, sine = tables(positions)
    vmem = pl.BlockSpec(memory_space=pltpu.VMEM)
    hbm = pl.BlockSpec(memory_space=pl.ANY)
    bf16 = jnp.bfloat16
    dma = pltpu.SemaphoreType.DMA
    heads = q_cols // HEAD_SIZE
    own, got = pl.pallas_call(
        functools.partial(layer_kernel, n_cp=n_cp, n_tp=n_tp, longest=longest),
        out_shape=(
            jax.ShapeDtypeStruct((tok, feat), bf16),
            jax.ShapeDtypeStruct((n_tp - 1, tok, feat), bf16),
        ),
        in_specs=[hbm] * 6 + [vmem, vmem, hbm],
        out_specs=(hbm, hbm),
        scratch_shapes=[
            pltpu.VMEM((n_tp, tok, feat), bf16),
            pltpu.VMEM((width, q_cols), bf16),
            pltpu.VMEM((seq, kv_cols), bf16),
            pltpu.VMEM((heads, tok, HEAD_SIZE), bf16),
            pltpu.VMEM((CHUNK, width), bf16),
            pltpu.VMEM((n_cp, 1, tok), jnp.int32),
            pltpu.VMEM((tok, LANES), bf16),
            pltpu.VMEM((1, width), jnp.float32),
            pltpu.VMEM((tok, feat), bf16),
            dma((n_tp - 1, chunks)),
            dma((n_tp - 1, chunks)),
            dma(()),
            dma((2,)),
            dma((3 + n_tp,)),
            dma((n_cp,)),
            dma((n_cp,)),
            dma((4, n_cp // 2 * chunks)),
            dma((n_cp * chunks,)),
            dma((n_tp - 1, n_tiles)),
            dma((n_tp - 1, n_tiles)),
            dma((n_tiles,)),
        ],
        compiler_params=pltpu.CompilerParams(
            collective_id=0, has_side_effects=True, vmem_limit_bytes=67_000_000
        ),
    )(
        hidden, norm_gain, w_query, w_key, w_value, w_out, cosine, sine, doc_ids,
    )
    total = own.astype(jnp.float32)
    for i in range(n_tp - 1):
        total = total + got[i].astype(jnp.float32)
    return total.astype(bf16)


def solution(mesh):
    in_specs = (
        P("cp", "tp"),
        P(),
        P(None, "tp"),
        P(None, "tp"),
        P(None, "tp"),
        P("tp", None),
        P("cp"),
    )
    body = functools.partial(shards, n_cp=mesh.shape["cp"], n_tp=mesh.shape["tp"])
    return jax.shard_map(
        body, mesh=mesh, in_specs=in_specs, out_specs=P("cp", "tp"), check_vma=False
    )
```
